32 devices in a mesh: owner: 8 (over z, y), kvh: 4 (over x, core).
Axes of the slice: x: 2, y: 2, z: 4, core: 2. Of those that a mesh axis runs over, the one named last changes fastest.
Arguments:
- queries: bfloat16 [16, 32, 32, 128], P('owner', None, 'kvh'), may hold values from -6 to 6
- new_keys: bfloat16 [16, 32, 4, 128], P('owner', None, 'kvh'), may hold values from -6 to 6
- new_values: bfloat16 [16, 32, 4, 128], P('owner', None, 'kvh'), may hold values from -6 to 6
- ancestors: int32 [16, 32], P('owner'), may hold values from 0 to 47, as said below
- tile_keys: bfloat16 [48, 4, 512, 128], P('owner', 'kvh'), may hold values from -6 to 6
- tile_values: bfloat16 [48, 4, 512, 128], P('owner', 'kvh'), may hold values from -6 to 6
- tile_lengths: int32 [48], P('owner'), may hold values from 2 to 512
- out_weight: bfloat16 [4096, 8192], P('kvh'), may hold values from -0.09375 to 0.09375
Outputs:
- mixed: bfloat16 [512, 8192], P(('owner', 'kvh'))
The draws below stay inside these ranges and needn't reach their ends.
Inputs may be any that keep to these rules, and one draw needn't show every extreme that they name: `ancestors`: each row names 32 different tiles.
All inputs are finite; a program needn't handle non-finite values.
Results may differ from the reference program's by a relative error of at most 0.017.
Values may be sent and summed in bfloat16 or wider, within the bound.
A program may use at most 320 MiB of HBM per device.

```python
import math
import jax
import jax.numpy as jnp
from jax import lax

D = 8192
HEAD = 128
QPG = 8
TILE = 512
HT = 32
NEW = 32
KVHEADS = 4
QHEADS = 32
PARTICLES = 16
TILES = 48
N_OWNER = 8


def ancestry(key):
    base_key = jax.random.fold_in(key, 11)
    spread_key = jax.random.fold_in(key, 12)
    favour = jax.random.randint(base_key, (TILES,), 0, 3) * 4096
    noise_part = jax.random.randint(spread_key, (PARTICLES, TILES), 0, 4096)
    scores_int = favour[None, :] + noise_part
    ordering = jnp.argsort(-scores_int, axis=1, stable=True)
    return ordering[:, :HT].astype(jnp.int32)


def draw_ancestors(key, part):
    return ancestry(key)


def drawn(key):
    coin_bits = jax.random.randint(jax.random.fold_in(key, 21), (KVHEADS, HEAD), 0, 2)
    sign_rows = (2 * coin_bits - 1).astype(jnp.float32)
    lead_row = 6.0 * sign_rows
    lowered_count = int(1.5 * math.sqrt(HEAD))
    lowered_mask = (jnp.arange(HEAD) < lowered_count).astype(jnp.float32)
    next_row = sign_rows * (6.0 - 0.25 * lowered_mask)[None, :]
    return (sign_rows, lead_row, next_row)


def chosen():
    return jnp.arange(PARTICLES) % 4 == 0


def normal_part(key, shape):
    return jnp.clip(jax.random.normal(key, shape, jnp.float32), -6.0, 6.0)


def draw_queries(key, part):
    values = normal_part(jax.random.fold_in(key, 31), (PARTICLES, NEW, QHEADS, HEAD))
    sign_rows, lead_row, next_row = drawn(key)
    levels = jnp.array([3.0, 4.0], jnp.float32)
    heads = jnp.arange(QHEADS)
    group_of = heads // QPG
    positions = jnp.arange(NEW)
    strength = levels[(group_of[None, :] + positions[:, None]) % levels.shape[0]]
    planted = sign_rows[group_of][None, :, :] * strength[:, :, None]
    token_hit = (positions == NEW - 1) | (positions == NEW // 2)
    head_hit = heads % QPG == 0
    selected = chosen()[:, None, None] & token_hit[None, :, None] & head_hit[None, None, :]
    return jnp.where(selected[..., None], planted[None], values).astype(jnp.bfloat16)


def draw_new_keys(key, part):
    values = normal_part(jax.random.fold_in(key, 32), (PARTICLES, NEW, KVHEADS, HEAD))
    sign_rows, lead_row, next_row = drawn(key)
    positions = jnp.arange(NEW)
    planted = jnp.where((positions == 0)[:, None, None], lead_row[None], next_row[None])
    selected = chosen()[:, None] & (positions < 2)[None, :]
    return jnp.where(selected[:, :, None, None], planted[None], values).astype(jnp.bfloat16)


def draw_tile_keys(key, part):
    values = normal_part(jax.random.fold_in(key, 33), (TILES, KVHEADS, TILE, HEAD))
    sign_rows, lead_row, next_row = drawn(key)
    history = ancestry(key)
    first_tiles = jnp.where(chosen(), history[:, 0], -1)
    planted_tiles = jnp.any(first_tiles[:, None] == jnp.arange(TILES)[None, :], axis=0)
    slots = jnp.arange(TILE)
    planted = jnp.where((slots == 0)[None, :, None], lead_row[:, None, :], next_row[:, None, :])
    selected = planted_tiles[:, None] & (slots < 2)[None, :]
    return jnp.where(selected[:, None, :, None], planted[None], values).astype(jnp.bfloat16)


def plant(result, key, smallest, top_value):
    longest = result.shape.index(max(result.shape))
    spots = []
    for shift in (0, 1):
        where = [jax.random.randint(jax.random.fold_in(key, axis), (), 0, length) for axis, length in enumerate(result.shape)]
        where[longest] = (where[longest] + shift) % result.shape[longest]
        spots.append(tuple(where))
    return result.at[spots[0]].set(smallest).at[spots[1]].set(top_value)


def level_of(key, shape, pieces, low, top_value):
    gain, own = 1.0, jax.random.fold_in(key, 6)
    for dim, parts in pieces:
        draws = jnp.exp(jax.random.uniform(jax.random.fold_in(own, dim), (parts,), jnp.float32, low / len(pieces), top_value / len(pieces)))
        gain = gain * jnp.repeat(draws, shape[dim] // parts).reshape([-1 if axis == dim else 1 for axis in range(len(shape))])
    return gain


def scatter_about(rng, shape, deviation, most, split=(), kind=jnp.bfloat16):
    factor_of = level_of(rng, shape, split, -0.22, 0.18) if split else 1.0
    drawn = jax.random.normal(rng, shape, jnp.float32) * deviation * factor_of
    return jnp.minimum(jnp.maximum(drawn, -most), most).astype(kind)


def setup_inputs(seed: int = 0) -> dict:
    key_list = jax.random.split(jax.random.key(seed), 9)
    queries = draw_queries(jax.random.fold_in(key_list[8], 71), 0)
    new_keys = draw_new_keys(jax.random.fold_in(key_list[8], 71), 0)
    new_values = scatter_about(key_list[2], (PARTICLES, NEW, KVHEADS, HEAD), 1.0, 6.0, ((0, 8), (2, 4)))
    ancestors = draw_ancestors(jax.random.fold_in(key_list[8], 71), 0)
    tile_keys = draw_tile_keys(jax.random.fold_in(key_list[8], 71), 0)
    tile_values = scatter_about(key_list[5], (TILES, KVHEADS, TILE, HEAD), 1.0, 6.0, ((0, 8), (1, 4)))
    tile_lengths = plant(jax.random.randint(key_list[6], (TILES,), 2, TILE + 1), jax.random.fold_in(key_list[6], 1), 2, TILE).astype(jnp.int32)
    out_weight = scatter_about(key_list[7], (QHEADS * HEAD, D), (QHEADS * HEAD) ** -0.5, 0.09375, ((0, 4),))
    return {"queries": queries, "new_keys": new_keys, "new_values": new_values, "ancestors": ancestors, "tile_keys": tile_keys, "tile_values": tile_values, "tile_lengths": tile_lengths, "out_weight": out_weight}


NEG = -1e30


def owner_partial(qrows, keys, values, live, member):
    count_p, rows, width = qrows.shape
    count, size = keys.shape[0], keys.shape[1]
    flat = qrows.reshape(count_p * rows, width)
    scores = jnp.dot(flat, keys.reshape(count * size, width).T, preferred_element_type=jnp.float32) * (width ** -0.5)
    scores = scores.reshape(count_p, rows, count * size)
    valid = jnp.repeat(member, size, axis=1)[:, None, :] & live.reshape(count * size)[None, None, :]
    masked = jnp.where(valid, scores, NEG)
    peak = jnp.max(masked, axis=2)
    weights = jnp.where(valid, jnp.exp(masked - peak[..., None]), 0.0)
    total = jnp.sum(weights, axis=2)
    summed = jnp.dot(weights.astype(jnp.bfloat16).reshape(count_p * rows, count * size),
                     values.reshape(count * size, width), preferred_element_type=jnp.float32)
    summed = summed.reshape(count_p, rows, width)
    safe = jnp.where(total > 0, total, 1.0)
    average = jnp.where(total[..., None] > 0, summed / safe[..., None], 0.0).astype(jnp.bfloat16)
    return average, peak, total


def self_partial(query, keys, values):
    count_p, new, group, width = query.shape
    scores = jnp.einsum('ntgh,nsh->ntgs', query.astype(jnp.float32), keys.astype(jnp.float32)) * (width ** -0.5)
    steps = jnp.arange(new)
    causal = (steps[:, None] >= steps[None, :])[None, :, None, :]
    masked = jnp.where(causal, scores, NEG)
    peak = jnp.max(masked, axis=3)
    weights = jnp.where(causal, jnp.exp(masked - peak[..., None]), 0.0)
    total = jnp.sum(weights, axis=3)
    summed = jnp.einsum('ntgs,nsh->ntgh', weights.astype(jnp.bfloat16).astype(jnp.float32), values.astype(jnp.float32))
    rows = new * group
    return summed.reshape(count_p, rows, width), peak.reshape(count_p, rows), total.reshape(count_p, rows)


def combine(own, average, peak, total):
    own_sum, own_peak, own_total = own
    top = jnp.maximum(own_peak, jnp.max(peak, axis=0))
    own_factor = jnp.exp(own_peak - top)
    factor = total * jnp.exp(peak - top[None])
    denom = own_total * own_factor + jnp.sum(factor, axis=0)
    numer = own_sum * own_factor[..., None] + jnp.sum(factor[..., None] * average.astype(jnp.float32), axis=0)
    return (numer / denom[..., None]).astype(jnp.bfloat16)


def reference(queries, new_keys, new_values, ancestors, tile_keys, tile_values, tile_lengths, out_weight):
    count_p, new, heads, width = queries.shape
    heads_kv = new_keys.shape[2]
    group = heads // heads_kv
    tiles, size = tile_keys.shape[0], tile_keys.shape[2]
    per_owner = tiles // N_OWNER
    member = jnp.any(ancestors[:, :, None] == jnp.arange(tiles, dtype=jnp.int32)[None, None, :], axis=1)
    member_own = member.reshape(count_p, N_OWNER, per_owner).transpose(1, 0, 2)
    live = jnp.arange(size, dtype=jnp.int32)[None, :] < tile_lengths[:, None]
    live_own = live.reshape(N_OWNER, per_owner, size)
    keys_own = tile_keys.reshape(N_OWNER, per_owner, heads_kv, size, width)
    values_own = tile_values.reshape(N_OWNER, per_owner, heads_kv, size, width)
    outputs = []
    for head in range(heads_kv):
        query = queries[:, :, head * group:(head + 1) * group, :]
        qrows = query.reshape(count_p, new * group, width)

        def one(items):
            return owner_partial(qrows, items[0], items[1], items[2], items[3])

        average, peak, total = lax.map(one, (keys_own[:, :, head], values_own[:, :, head], live_own, member_own))
        own = self_partial(query, new_keys[:, :, head], new_values[:, :, head])
        outputs.append(combine(own, average, peak, total).reshape(count_p, new, group * width))
    attention = jnp.concatenate(outputs, axis=2).reshape(count_p * new, heads * width)
    return jnp.dot(attention, out_weight, preferred_element_type=jnp.float32).astype(jnp.bfloat16)
```

```python
import functools
import math

import jax
import jax.numpy as jnp
from jax import lax
from jax.experimental import pallas as pl
from jax.experimental.pallas import tpu as pltpu
from jax.sharding import PartitionSpec as P

NEG = -1e30
LANES = 128
MESH = pl.DeviceIdType.MESH


def split_axis(n):
    fast = 1
    while fast * fast * 4 <= n and n % (fast * 2) == 0:
        fast *= 2
    if fast == 1 and n % 2 == 0:
        fast = 2
    return n // fast, fast


def remote(src, dst, send, recv, owner, kvh):
    return pltpu.make_async_remote_copy(
        src_ref=src, dst_ref=dst, send_sem=send, recv_sem=recv,
        device_id=(owner, kvh), device_id_type=MESH,
    )


def greet(peers):
    barrier = pltpu.get_barrier_semaphore()
    for peer in peers:
        pl.semaphore_signal(barrier, inc=1, device_id=peer, device_id_type=MESH)
    pl.semaphore_wait(barrier, len(peers))


def gather_kernel(slow, fast, q_ref, m_ref, qo, mo, qs, qr, ms, mr, ls):
    me, k = lax.axis_index("owner"), lax.axis_index("kvh")
    a, b = lax.div(me, fast), lax.rem(me, fast)
    line = [None] + [lax.rem(a + i, slow) * fast + b for i in range(1, slow)]
    side = [None] + [a * fast + lax.rem(b + j, fast) for j in range(1, fast)]
    local = [
        pltpu.make_async_copy(q_ref, qo.at[me], ls.at[0]),
        pltpu.make_async_copy(m_ref, mo.at[me], ls.at[1]),
    ]
    for copy in local:
        copy.start()
    greet([(d, k) for d in line[1:] + side[1:]])

    def pair(src_q, src_m, at, index, target):
        return [
            remote(src_m, mo.at[at], ms.at[index], mr.at[index], target, k),
            remote(src_q, qo.at[at], qs.at[index], qr.at[index], target, k),
        ]

    sent, first = [], [None]
    for i in range(1, slow):
        copies = pair(q_ref, m_ref, me, i * fast, line[i])
        first.append(copies)
        sent += copies
        for copy in copies:
            copy.start()
    later = []
    for j in range(1, fast):
        copies = pair(q_ref, m_ref, me, j, side[j])
        later += copies
        for copy in copies:
            copy.start()
    for i in range(1, slow):
        for copy in first[i]:
            copy.wait_recv()
        source = lax.rem(a + slow - i, slow) * fast + b
        for j in range(1, fast):
            copies = pair(qo.at[source], mo.at[source], source, i * fast + j, side[j])
            later += copies
            for copy in copies:
                copy.start()
    for copy in later:
        copy.wait_recv()
    for copy in sent + later:
        copy.wait_send()
    for copy in local:
        copy.wait()


def to_row(column):
    size = column.shape[0]
    rows = lax.broadcasted_iota(jnp.int32, (size, size), 0)
    cols = lax.broadcasted_iota(jnp.int32, (size, size), 1)
    wide = jnp.broadcast_to(column, (size, size))
    return jnp.sum(jnp.where(rows == cols, wide, 0.0), axis=0, keepdims=True)


def to_column(row):
    size = row.shape[1]
    rows = lax.broadcasted_iota(jnp.int32, (size, size), 0)
    cols = lax.broadcasted_iota(jnp.int32, (size, size), 1)
    wide = jnp.broadcast_to(row, (size, size))
    return jnp.sum(jnp.where(rows == cols, wide, 0.0), axis=1, keepdims=True)


def attend_kernel(
    part_dev, group, mem, lens, me_ref, q_ref, k_ref, v_ref, nk_ref, nv_ref,
    avg_ref, lse_ref, top, mass, acc,
):
    p = pl.program_id(0)
    me = me_ref[0]
    per_owner, size, width = k_ref.shape
    rows = q_ref.shape[1]
    scale = width ** (-0.5)
    rate = scale * math.log2(math.e)
    top[...] = jnp.full(top.shape, NEG, jnp.float32)
    mass[...] = jnp.zeros(mass.shape, jnp.float32)
    acc[...] = jnp.zeros(acc.shape, jnp.float32)
    home, place = lax.div(p, part_dev), lax.rem(p, part_dev)

    def fold(keys, values, valid):
        scores = lax.dot_general(
            q_ref[0], keys, (((1,), (1,)), ((), ())), preferred_element_type=jnp.float32
        )
        span = scores.shape[1]
        scores = jnp.where(valid, scores, NEG)
        old = top[:, :1]
        new = jnp.maximum(old, jnp.max(scores, axis=1, keepdims=True))
        decay = jnp.exp2((old - new) * rate)
        weights = jnp.exp2((scores - new) * rate)
        if span % LANES == 0:
            part = weights[:, :LANES]
            for c in range(1, span // LANES):
                part = part + weights[:, c * LANES : (c + 1) * LANES]
            mass[...] = mass[...] * decay + part
        else:
            one = lax.broadcasted_iota(jnp.int32, mass.shape, 1) == 0
            part = jnp.sum(weights, axis=1, keepdims=True)
            mass[...] = mass[...] * decay + jnp.where(one, part, 0.0)
        acc[...] = acc[...] * decay + jnp.dot(
            weights.astype(jnp.bfloat16), values, preferred_element_type=jnp.float32
        )
        top[...] = jnp.broadcast_to(new, top.shape)

    @pl.when(home == me)
    def _():
        new = nk_ref.shape[1]
        row = lax.broadcasted_iota(jnp.int32, (rows, new), 0)
        col = lax.broadcasted_iota(jnp.int32, (rows, new), 1)
        fold(nk_ref[place], nv_ref[place], row >= col * group)

    spans = [size]
    if size % (2 * LANES) == 0:
        spans = [size // 2, size]

    def tile(j, carry):
        member = mem[home * 8 + place, me * per_owner + j] > 0
        length = lens[j]
        low = 0
        for span in spans:
            fits = jnp.logical_and(length > low, length <= span)

            @pl.when(jnp.logical_and(member, fits))
            def _():
                slot = lax.broadcasted_iota(jnp.int32, (1, span), 1)
                fold(k_ref[j, :span], v_ref[j, :span], slot < length)

            low = span
        return carry

    lax.fori_loop(0, per_owner, tile, 0)
    total = jnp.sum(mass[...], axis=1, keepdims=True)
    some = total > 0
    safe = jnp.where(some, total, 1.0)
    avg_ref[0] = jnp.where(some, acc[...] / safe, 0.0).astype(jnp.bfloat16)
    logs = jnp.where(some, top[:, :1] * scale + jnp.log(safe), NEG)
    for r in range(rows // LANES):
        lse_ref[0, r : r + 1, :] = to_row(logs[r * LANES : (r + 1) * LANES])


def finish_kernel(
    slow, fast, outer, chunks, group, avg, lse, w, out,
    wbuf, r1a, r1l, s2a, s2l, r2a, r2l, wide, att, pb, r3, s4, r4,
    wsem, sa1, ra1, sl1, rl1, sa2, ra2, sl2, rl2, p3s, p3r, p4s, p4r,
):
    me, k = lax.axis_index("owner"), lax.axis_index("kvh")
    a, b = lax.div(me, fast), lax.rem(me, fast)
    x, core = lax.div(k, 2), lax.rem(k, 2)
    columns = wbuf.shape[2]

    def weight(c):
        at = pl.ds(pl.multiple_of(c * columns, columns), columns)
        return pltpu.make_async_copy(w.at[:, at], wbuf.at[c], wsem.at[c])

    for c in range(chunks):
        weight(c).start()
    line = [None] + [lax.rem(a + i, slow) * fast + b for i in range(1, slow)]
    side = [None] + [a * fast + lax.rem(b + j, fast) for j in range(1, fast)]
    partner = x * 2 + 1 - core
    across = [None] + [lax.rem(x + i, outer) * 2 + core for i in range(1, outer)]
    greet(
        [(d, k) for d in line[1:] + side[1:]]
        + [(me, partner)]
        + [(me, d) for d in across[1:]]
    )
    order = list(range(1, slow)) + [0]
    one = {}
    for i in order:
        for j in range(1, fast):
            block = lax.rem(a + i, slow) * fast + lax.rem(b + j, fast)
            one[i, j] = [
                remote(lse.at[block], r1l.at[j - 1, i], sl1.at[j - 1, i], rl1.at[j - 1, i], side[j], k),
                remote(avg.at[block], r1a.at[j - 1, i], sa1.at[j - 1, i], ra1.at[j - 1, i], side[j], k),
            ]
            for copy in one[i, j]:
                copy.start()

    per = avg.shape[1] // lse.shape[1] // LANES

    def merge(c, parts):
        place, r = lax.div(c, per), lax.rem(c, per)
        at = pl.ds(pl.multiple_of(c * LANES, LANES), LANES)
        logs = [to_column(l[place, pl.ds(r, 1), :]) for _, l in parts]
        peak = functools.reduce(jnp.maximum, logs)
        factors = [jnp.exp(l - peak) for l in logs]
        denom = functools.reduce(jnp.add, factors)
        numer = functools.reduce(
            jnp.add, [f * v[at, :].astype(jnp.float32) for f, (v, _) in zip(factors, parts)]
        )
        return place, r, at, numer / denom, peak + jnp.log(denom)

    pieces = avg.shape[1] // LANES
    two = [None]
    for i in order:
        for j in range(1, fast):
            for copy in one[i, j]:
                copy.wait_recv()
        block = lax.rem(a + i, slow) * fast + b
        parts = [(avg.at[block], lse.at[block])]
        parts += [(r1a.at[j - 1, i], r1l.at[j - 1, i]) for j in range(1, fast)]

        def step(c, carry, parts=parts, i=i):
            place, r, at, mean, logs = merge(c, parts)
            s2a[i, at, :] = mean.astype(jnp.bfloat16)
            s2l[i, place, pl.ds(r, 1), :] = to_row(logs)
            return carry

        lax.fori_loop(0, pieces, step, 0)
        if i:
            copies = [
                remote(s2l.at[i], r2l.at[i], sl2.at[i], rl2.at[i], line[i], k),
                remote(s2a.at[i], r2a.at[i], sa2.at[i], ra2.at[i], line[i], k),
            ]
            two.append(copies)
            for copy in copies:
                copy.start()
    for i in range(1, slow):
        for copy in two[i]:
            copy.wait_recv()
    parts = [(s2a.at[0], s2l.at[0])] + [(r2a.at[i], r2l.at[i]) for i in range(1, slow)]

    def last(c, carry):
        _, _, at, mean, _ = merge(c, parts)
        wide[at, :] = mean
        return carry

    lax.fori_loop(0, pieces, last, 0)
    tokens, width = att.shape[0], avg.shape[2]
    for g in range(group):
        att[:, g * width : (g + 1) * width] = wide[pl.ds(g, tokens, stride=group), :].astype(
            jnp.bfloat16
        )
    own = out.shape[0]

    def swap(c):
        return remote(pb.at[c, 1 - core], r3.at[c], p3s.at[c], p3r.at[c], me, partner)

    def spread(c, i):
        return remote(s4.at[c, i], r4.at[c, i], p4s.at[c, i], p4r.at[c, i], me, across[i])

    def project(c):
        weight(c).wait()
        part = jnp.dot(att[...], wbuf[c], preferred_element_type=jnp.float32)
        for d in range(2 * outer):
            pb[c, d % 2, d // 2] = part[d * own : (d + 1) * own].astype(jnp.bfloat16)
        swap(c).start()

    def pass_on(c):
        swap(c).wait_recv()
        for i in range(1, outer):
            to = lax.rem(x + i, outer)
            both = pb[c, core, to].astype(jnp.float32) + r3[c, to].astype(jnp.float32)
            s4[c, i] = both.astype(jnp.bfloat16)
            spread(c, i).start()

    project(0)

    def body(c, carry):
        project(c)
        pass_on(c - 1)
        return carry

    lax.fori_loop(1, chunks, body, 0)
    pass_on(chunks - 1)

    def close(c, carry):
        both = pb[c, core, x].astype(jnp.float32) + r3[c, x].astype(jnp.float32)
        for i in range(1, outer):
            spread(c, i).wait_recv()
            both = both + r4[c, i].astype(jnp.float32)
        at = pl.ds(pl.multiple_of(c * columns, columns), columns)
        out[:, at] = both.astype(jnp.bfloat16)
        swap(c).wait_send()
        for i in range(1, outer):
            spread(c, i).wait_send()
        return carry

    lax.fori_loop(0, chunks, close, 0)
    for copies in list(one.values()) + two[1:]:
        for copy in copies:
            copy.wait_send()


def local(
    queries, new_keys, new_values, ancestors, tile_keys, tile_values, tile_lengths, out_weight
):
    owners, heads = lax.axis_size("owner"), lax.axis_size("kvh")
    part_dev, new, group, width = queries.shape
    per_owner, size = tile_keys.shape[0], tile_keys.shape[2]
    tiles = per_owner * owners
    rows = new * group
    block = part_dev * rows
    slow, fast = split_axis(owners)
    padded = -(-tiles // LANES) * LANES
    bf16, f32, i32 = jnp.bfloat16, jnp.float32, jnp.int32
    dma = pltpu.SemaphoreType.DMA
    vmem = pl.BlockSpec(memory_space=pltpu.VMEM)

    member = jnp.any(
        ancestors[:, :, None] == jnp.arange(padded, dtype=i32)[None, None, :], axis=1
    ).astype(i32)
    member = jnp.pad(member, ((0, 8 - part_dev), (0, 0)))
    shared_q, shared_m = pl.pallas_call(
        functools.partial(gather_kernel, slow, fast),
        out_shape=(
            jax.ShapeDtypeStruct((owners, block, width), bf16),
            jax.ShapeDtypeStruct((owners, 8, padded), i32),
        ),
        in_specs=[vmem, vmem],
        out_specs=(vmem, vmem),
        scratch_shapes=[dma((owners,))] * 4 + [dma((2,))],
        compiler_params=pltpu.CompilerParams(collective_id=0, has_side_effects=True),
        name="gather",
    )(queries.reshape(block, width), member)

    count = owners * part_dev
    me = lax.axis_index("owner").astype(i32).reshape(1)
    whole3 = lambda p, *_: (0, 0, 0)
    each = lambda p, *_: (p, 0, 0)
    average, logs = pl.pallas_call(
        functools.partial(attend_kernel, part_dev, group),
        out_shape=(
            jax.ShapeDtypeStruct((count, rows, width), bf16),
            jax.ShapeDtypeStruct((count, 8, LANES), f32),
        ),
        grid_spec=pltpu.PrefetchScalarGridSpec(
            num_scalar_prefetch=3,
            grid=(count,),
            in_specs=[
                pl.BlockSpec((1, rows, width), each),
                pl.BlockSpec((per_owner, size, width), whole3),
                pl.BlockSpec((per_owner, size, width), whole3),
                pl.BlockSpec((part_dev, new, width), whole3),
                pl.BlockSpec((part_dev, new, width), whole3),
            ],
            out_specs=(
                pl.BlockSpec((1, rows, width), each),
                pl.BlockSpec((1, 8, LANES), each),
            ),
            scratch_shapes=[pltpu.VMEM((rows, LANES), f32), pltpu.VMEM((rows, LANES), f32),
                            pltpu.VMEM((rows, width), f32)],
        ),
        name="attend",
    )(
        shared_m.reshape(owners * 8, padded), tile_lengths, me,
        shared_q.reshape(count, rows, width), tile_keys[:, 0], tile_values[:, 0],
        new_keys[:, :, 0], new_values[:, :, 0],
    )

    depth, model = out_weight.shape
    outer = heads // 2
    chunks = 8
    columns = model // chunks
    tokens = part_dev * new
    own = tokens // heads
    return pl.pallas_call(
        functools.partial(finish_kernel, slow, fast, outer, chunks, group),
        out_shape=jax.ShapeDtypeStruct((own, model), bf16),
        in_specs=[vmem, vmem, pl.BlockSpec(memory_space=pl.ANY)],
        out_specs=vmem,
        scratch_shapes=[
            pltpu.VMEM((chunks, depth, columns), bf16),
            pltpu.VMEM((max(fast - 1, 1), slow, block, width), bf16),
            pltpu.VMEM((max(fast - 1, 1), slow, part_dev, 8, LANES), f32),
            pltpu.VMEM((slow, block, width), bf16),
            pltpu.VMEM((slow, part_dev, 8, LANES), f32),
            pltpu.VMEM((slow, block, width), bf16),
            pltpu.VMEM((slow, part_dev, 8, LANES), f32),
            pltpu.VMEM((block, width), f32),
            pltpu.VMEM((tokens, depth), bf16),
            pltpu.VMEM((chunks, 2, outer, own, columns), bf16),
            pltpu.VMEM((chunks, outer, own, columns), bf16),
            pltpu.VMEM((chunks, outer, own, columns), bf16),
            pltpu.VMEM((chunks, outer, own, columns), bf16),
            dma((chunks,)),
        ]
        + [dma((max(fast - 1, 1), slow))] * 4
        + [dma((slow,))] * 4
        + [dma((chunks,))] * 2
        + [dma((chunks, outer))] * 2,
        compiler_params=pltpu.CompilerParams(collective_id=1, has_side_effects=True),
        name="finish",
    )(
        average.reshape(owners, block, width),
        logs.reshape(owners, part_dev, 8, LANES),
        out_weight,
    )


def solution(mesh):
    return jax.shard_map(
        local,
        mesh=mesh,
        in_specs=(
            P("owner", None, "kvh", None),
            P("owner", None, "kvh", None),
            P("owner", None, "kvh", None),
            P("owner", None),
            P("owner", "kvh", None, None),
            P("owner", "kvh", None, None),
            P("owner"),
            P("kvh", None),
        ),
        out_specs=P(("owner", "kvh"), None),
        check_vma=False,
    )
```
